32 devices in a mesh: head: 4 (over z), ctx: 8 (over y, x, core).
Axes of the slice: x: 2, y: 2, z: 4, core: 2. Of those that a mesh axis runs over, the one named last changes fastest.
Arguments:
- queries: bfloat16 [8192, 4, 128], P('ctx', 'head'), may hold values from -120 to 120
- keys: bfloat16 [8192, 4, 128], P('ctx', 'head'), may hold values from -6 to 6
- values: bfloat16 [8192, 4, 128], P('ctx', 'head'), may hold values from -6 to 6
- house: bfloat16 [8192, 4, 128], P('ctx', 'head'), may hold values from -6 to 6
- rates: float32 [4, 8192], P('head', 'ctx'), may hold values from 0.0002 to 1.9, as said below
- out_weight: bfloat16 [512, 8192], P('head'), may hold values from -0.375 to 0.375
Outputs:
- attended: bfloat16 [8192, 4, 128], P('ctx', 'head')
- projected: bfloat16 [8192, 8192], P('ctx', 'head')
The draws below stay inside these ranges and needn't reach their ends.
Inputs may be any that keep to these rules, and one draw needn't show every extreme that they name: `rates`: strictly positive and below 2, so every transition is a contraction.
All inputs are finite; a program needn't handle non-finite values.
Results may differ from the reference program's by a relative error of at most 0.015.
Values may be sent and summed in bfloat16 or wider, within the bound.
A program may use at most 64 MiB of HBM per device.

```python
import jax
import jax.numpy as jnp
from jax import lax

DH = 128
DMODEL = 8192
BLOCK = 128
TOK_DEV = 1024
SHARD_ATTN_COUNT = 4
PROMPT_LENGTH = 8192
N_CTX = 8


def key_base(key):
    return jnp.clip(jax.random.normal(jax.random.fold_in(key, 31), (PROMPT_LENGTH, SHARD_ATTN_COUNT, DH), jnp.float32), -6.0, 6.0)


def draw_keys(key, part):
    return key_base(key).astype(jnp.bfloat16)


def draw_queries(key, part):
    drawn = jnp.clip(2.0 * jax.random.normal(jax.random.fold_in(key, 47), (PROMPT_LENGTH, SHARD_ATTN_COUNT, DH), jnp.float32), -12.0, 12.0)
    return drawn.astype(jnp.bfloat16)


def draw_rates(key, part):
    head_key = jax.random.fold_in(key, 61)
    jitter_key = jax.random.fold_in(key, 67)
    spike_draw_seed = jax.random.fold_in(key, 71)
    spot_key = jax.random.fold_in(key, 73)
    lowest, highest = (0.002, 0.6)
    head_rate = jnp.exp(jax.random.uniform(head_key, (SHARD_ATTN_COUNT, 1), jnp.float32, jnp.log(lowest), jnp.log(highest)))
    random_noise = jnp.exp(jax.random.uniform(jitter_key, (SHARD_ATTN_COUNT, PROMPT_LENGTH), jnp.float32, jnp.log(0.5), jnp.log(2.0)))
    spots = jax.random.randint(spot_key, (6,), 0, PROMPT_LENGTH)
    position = jnp.arange(PROMPT_LENGTH)
    struck = jnp.any(position[:, None] == spots[None, :], axis=1)
    steep_forgetting = jax.random.uniform(spike_draw_seed, (SHARD_ATTN_COUNT, PROMPT_LENGTH), jnp.float32, 0.8, 1.5)
    steady = jnp.clip(head_rate * random_noise, 0.0002, 1.9)
    return jnp.where(struck[None, :], steep_forgetting, steady).astype(jnp.float32)


def spiked(values, key, source, target, parts, factor):
    owner, partner = [(jnp.arange(values.shape[dim]) // (values.shape[dim] // parts)).reshape([-1 if axis == dim else 1 for axis in range(values.ndim)]) for dim in (source, target)]
    chosen = jax.random.permutation(key, parts)[partner]
    strong = (owner == chosen) | (owner == (partner + parts // 2) % parts)
    return jnp.where(strong, factor * values, values)


def block_scale(key, shape, split, least, largest):
    def one(dim, parts):
        steps = jax.random.uniform(jax.random.fold_in(jax.random.fold_in(key, 6), dim), (parts,), jnp.float32, least / len(split), largest / len(split))
        return jnp.repeat(jnp.exp(steps), shape[dim] // parts).reshape((-1,) + (1,) * (len(shape) - dim - 1))

    loudness = one(*split[0])
    for cut in split[1:]:
        loudness = loudness * one(*cut)
    return loudness


def centred(rng, shape, deviation, bound, pieces=(), kind=jnp.bfloat16):
    loudness = block_scale(rng, shape, pieces, -0.22, 0.18) if pieces else 1.0
    drawn = jax.random.normal(rng, shape, jnp.float32) * deviation * loudness
    return jnp.minimum(jnp.maximum(drawn, -bound), bound).astype(kind)


def heavy_noise(key, shape, spread, bound, shards, heavy, held_as=jnp.bfloat16):
    values = spread * jax.random.normal(key, shape, jnp.float32)
    if shards:
        values = values * block_scale(key, shape, shards, -0.22, 0.18)
    return jnp.clip(spiked(values, jax.random.fold_in(key, 3), *heavy), -bound, bound).astype(held_as)


def setup_inputs(seed: int = 0) -> dict:
    streams_of = jax.random.split(jax.random.key(seed), 7)
    return {
        "queries": draw_queries(jax.random.fold_in(streams_of[6], 71), 0),
        "keys": draw_keys(jax.random.fold_in(streams_of[6], 71), 0),
        "values": centred(streams_of[2], (PROMPT_LENGTH, SHARD_ATTN_COUNT, DH), 1.0, 6.0, ((0, 8), (1, 4))),
        "house": centred(streams_of[3], (PROMPT_LENGTH, SHARD_ATTN_COUNT, DH), 1.0, 6.0, ((0, 8), (1, 4))),
        "rates": draw_rates(jax.random.fold_in(streams_of[6], 71), 0),
        "out_weight": heavy_noise(streams_of[5], (SHARD_ATTN_COUNT * DH, DMODEL), (SHARD_ATTN_COUNT * DH) ** -0.5, 0.375, ((0, 4),), (0, 1, 4, 2.0)),
    }


EPSILON = 1e-06
NEGATIVE = -1e+30
PRECISE = lax.Precision.HIGHEST

def matmul(first_matrix, second_matrix):
    return jnp.matmul(first_matrix, second_matrix, precision=PRECISE)

def block_parts(query_rows, key_rows, house_rows, decays):
    length = query_rows.shape[0]
    features = query_rows.shape[1]
    row_index = lax.broadcasted_iota(jnp.int32, (length, length), 0)
    col_index = lax.broadcasted_iota(jnp.int32, (length, length), 1)
    gram_matrix = matmul(house_rows, house_rows.T)
    zero_block = jnp.zeros_like(gram_matrix)
    lower_part = jnp.where(row_index > col_index, gram_matrix, zero_block) + jnp.diag(1.0 / decays)
    identity = jnp.eye(length, dtype=query_rows.dtype)
    inverse = jax.scipy.linalg.solve_triangular(lower_part, identity, lower=True)
    left_part = jnp.where(row_index >= col_index, matmul(query_rows, house_rows.T), zero_block)
    right_part = matmul(inverse, jnp.where(row_index > col_index, matmul(house_rows, key_rows.T), zero_block))
    start_query = query_rows - matmul(matmul(left_part, inverse), house_rows)
    final_key = key_rows - matmul(right_part.T, house_rows)
    inside_mask = matmul(query_rows, key_rows.T) - matmul(left_part, right_part)
    inside_mask = jnp.where(row_index >= col_index, inside_mask, NEGATIVE)
    passage = jnp.eye(features, dtype=query_rows.dtype) - matmul(house_rows.T, matmul(inverse, house_rows))
    return (start_query, final_key, inside_mask, passage)

def shard_local(start_query, final_key, inside_mask, passage):
    blocks, length, features = start_query.shape
    rows_dev = blocks * length
    col_block = lax.broadcasted_iota(jnp.int32, (length, rows_dev), 1) // length
    anchor = jnp.zeros((), jnp.int32)

    def advance(running, element):
        moved_keys, prefix = running
        number, query_rows, key_rows, inside_rows, passage_rows = element
        across = matmul(query_rows, moved_keys.T)
        scores = jnp.where(col_block < number, across, NEGATIVE)
        scores = lax.dynamic_update_slice(scores, inside_rows, (anchor, number * length))
        carried_query = matmul(query_rows, prefix)
        moved_keys = matmul(moved_keys, passage_rows.T)
        moved_keys = lax.dynamic_update_slice(moved_keys, key_rows, (number * length, anchor))
        prefix = matmul(passage_rows, prefix)
        return ((moved_keys, prefix), (scores, carried_query))
    numbers = jnp.arange(blocks, dtype=jnp.int32)
    initial = (jnp.zeros((rows_dev, features), start_query.dtype), jnp.eye(features, dtype=start_query.dtype))
    (end_keys, transit), (scores, carried) = lax.scan(advance, initial, (numbers, start_query, final_key, inside_mask, passage))
    return (scores.reshape(rows_dev, rows_dev), carried.reshape(rows_dev, features), end_keys, transit)

def head_attention(query_all, key_all, value_all, house_all, decays):
    features = query_all.shape[1]
    blocks = PROMPT_LENGTH // BLOCK
    query_f = query_all.astype(jnp.float32) * features ** (-0.5)
    key_f = key_all.astype(jnp.float32)
    house_f = house_all.astype(jnp.float32)
    house_unit = house_f / jnp.sqrt(lax.optimization_barrier(jnp.sum(house_f * house_f, axis=1, keepdims=True)) + EPSILON)
    block_data = jax.vmap(block_parts)(query_f.reshape(blocks, BLOCK, features), key_f.reshape(blocks, BLOCK, features), house_unit.reshape(blocks, BLOCK, features), decays.reshape(blocks, BLOCK))
    per_shard = [array.reshape((N_CTX, TOK_DEV // BLOCK) + array.shape[1:]) for array in block_data]
    scores_local, carried, end_keys, transit = jax.vmap(shard_local)(*per_shard)
    stored_keys = end_keys.astype(jnp.bfloat16).astype(jnp.float32)
    value_blocks = value_all.astype(jnp.float32).reshape(N_CTX, TOK_DEV, features)
    anchor = jnp.zeros((), jnp.int32)

    def shard_rows(number):
        start_rows = lax.dynamic_index_in_dim(carried, number, 0, keepdims=False)
        own_scores = lax.dynamic_index_in_dim(scores_local, number, 0, keepdims=False)
        row_scores = jnp.full((TOK_DEV, PROMPT_LENGTH), NEGATIVE, query_f.dtype)
        row_scores = lax.dynamic_update_slice(row_scores, own_scores, (anchor, number * TOK_DEV))

        def visit_shard(offset, running):
            moving, table_scores = running
            source = number - 1 - offset
            block_keys = lax.dynamic_index_in_dim(stored_keys, source, 0, keepdims=False)
            table_scores = lax.dynamic_update_slice(table_scores, matmul(moving, block_keys.T), (anchor, source * TOK_DEV))
            moving = matmul(moving, lax.dynamic_index_in_dim(transit, source, 0, keepdims=False))
            return (moving, table_scores)
        _, row_scores = lax.fori_loop(anchor, number, visit_shard, (start_rows, row_scores))
        row_peak = lax.optimization_barrier(jnp.max(row_scores, axis=1, keepdims=True))
        weight_matrix = jnp.exp(row_scores - row_peak)
        totals = lax.optimization_barrier(jnp.sum(weight_matrix, axis=1))
        rounded = lax.optimization_barrier(weight_matrix.astype(jnp.bfloat16)).astype(jnp.float32)

        def gather_values(source, summed):
            weight_piece = lax.dynamic_slice_in_dim(rounded, source * TOK_DEV, TOK_DEV, 1)
            value_piece = lax.dynamic_index_in_dim(value_blocks, source, 0, keepdims=False)
            return summed + matmul(weight_piece, value_piece)
        summed = lax.fori_loop(anchor, number + 1, gather_values, jnp.zeros((TOK_DEV, features), query_f.dtype))
        return (summed / totals[:, None]).astype(jnp.bfloat16)
    outputs = lax.map(shard_rows, jnp.arange(N_CTX, dtype=jnp.int32))
    return outputs.reshape(PROMPT_LENGTH, features)

def reference(queries, keys, values, house, rates, out_weight):

    def select_head(number):
        return head_attention(lax.dynamic_index_in_dim(queries, number, 1, keepdims=False), lax.dynamic_index_in_dim(keys, number, 1, keepdims=False), lax.dynamic_index_in_dim(values, number, 1, keepdims=False), lax.dynamic_index_in_dim(house, number, 1, keepdims=False), lax.dynamic_index_in_dim(rates, number, 0, keepdims=False))
    per_head = lax.map(select_head, jnp.arange(SHARD_ATTN_COUNT, dtype=jnp.int32))
    attended = jnp.transpose(per_head, (1, 0, 2))
    flattened = attended.reshape(PROMPT_LENGTH, SHARD_ATTN_COUNT * DH)
    projected = matmul(flattened.astype(jnp.float32), out_weight.astype(jnp.float32))
    return (attended, projected.astype(jnp.bfloat16))
```

```python
import functools

import jax
import jax.numpy as jnp
from jax import lax
from jax.experimental import pallas as pl
from jax.experimental.pallas import tpu as pltpu
from jax.sharding import PartitionSpec as P

EPSILON = 1e-06
NEGATIVE = -1e30
MESH = pl.DeviceIdType.MESH
F32 = jnp.float32
BF16 = jnp.bfloat16


def mm(a, b):
    return jnp.dot(a, b, preferred_element_type=F32)


def split(x):
    high = x.astype(BF16)
    return high, (x - high.astype(F32)).astype(BF16)


def dot3(a, b):
    (ah, al), (bh, bl) = split(a), split(b)
    if a.shape[1] <= 128:
        return mm(jnp.concatenate([ah, al], 1), jnp.concatenate([bh, bh], 0)) + mm(ah, bl)
    return mm(ah, bh) + mm(al, bh) + mm(ah, bl)


def kernel(
    n_ctx, n_head, block,
    q_ref, k_ref, v_ref, h_ref, rates_ref, w_ref,
    att_ref, flat_ref, cols_ref,
    kall, vall, tall, ksend, tsend, nmat, inv, moved, mov, acc, peak, total,
    v_ssem, v_rsem, k_ssem, k_rsem, t_ssem, t_rsem, w_ssem, w_rsem, a_ssem, a_rsem, loc_sem,
):
    me = lax.axis_index("ctx")
    head = lax.axis_index("head")
    rows, feat = q_ref.shape
    blocks = rows // block
    width = cols_ref.shape[1]
    scale = feat ** (-0.5)

    barrier = pltpu.get_barrier_semaphore()
    for step in range(1, n_ctx):
        pl.semaphore_signal(barrier, inc=1, device_id={"ctx": lax.rem(me + step, n_ctx)}, device_id_type=MESH)
    for step in range(1, n_head):
        pl.semaphore_signal(barrier, inc=1, device_id={"head": lax.rem(head + step, n_head)}, device_id_type=MESH)
    pl.semaphore_wait(barrier, n_ctx + n_head - 2)

    def v_copy(owner, peer):
        return pltpu.make_async_remote_copy(
            src_ref=v_ref, dst_ref=vall.at[owner], send_sem=v_ssem.at[peer], recv_sem=v_rsem.at[owner],
            device_id={"ctx": peer}, device_id_type=MESH)

    def k_copy(owner, peer):
        return pltpu.make_async_remote_copy(
            src_ref=ksend, dst_ref=kall.at[owner], send_sem=k_ssem.at[peer], recv_sem=k_rsem.at[owner],
            device_id={"ctx": peer}, device_id_type=MESH)

    def t_copy(owner, peer):
        return pltpu.make_async_remote_copy(
            src_ref=tsend, dst_ref=tall.at[owner], send_sem=t_ssem.at[peer], recv_sem=t_rsem.at[owner],
            device_id={"ctx": peer}, device_id_type=MESH)

    def w_copy(owner, peer):
        return pltpu.make_async_remote_copy(
            src_ref=w_ref.at[:, pl.ds(pl.multiple_of(peer * width, 128), width)],
            dst_ref=cols_ref.at[pl.ds(pl.multiple_of(owner * feat, 128), feat), :],
            send_sem=w_ssem.at[peer], recv_sem=w_rsem.at[owner],
            device_id={"head": peer}, device_id_type=MESH)

    def a_copy(owner, peer):
        return pltpu.make_async_remote_copy(
            src_ref=att_ref, dst_ref=flat_ref.at[:, pl.ds(pl.multiple_of(owner * feat, 128), feat)],
            send_sem=a_ssem.at[peer], recv_sem=a_rsem.at[owner],
            device_id={"head": peer}, device_id_type=MESH)

    def later(action):
        def go(peer, carry):
            action(peer)
            return carry
        lax.fori_loop(me + 1, n_ctx, go, 0)

    later(lambda peer: v_copy(me, peer).start())
    for step in range(1, n_head):
        w_copy(head, lax.rem(head + step, n_head)).start()
    w_own = pltpu.make_async_copy(
        w_ref.at[:, pl.ds(pl.multiple_of(head * width, 128), width)],
        cols_ref.at[pl.ds(pl.multiple_of(head * feat, 128), feat), :], loc_sem.at[0])
    w_own.start()

    ri = lax.broadcasted_iota(jnp.int32, (block, block), 0)
    ci = lax.broadcasted_iota(jnp.int32, (block, block), 1)
    eye = ri == ci
    strict = ri > ci
    nt = (((1,), (1,)), ((), ()))

    scales = []
    for b in range(blocks):
        part = slice(b * block, (b + 1) * block)
        hb = h_ref[part, :]
        gram = lax.dot_general(hb, hb, nt, preferred_element_type=F32)
        diag = jnp.where(eye, gram, 0.0)
        r_col = lax.rsqrt(jnp.sum(diag, axis=1, keepdims=True) + EPSILON)
        r_row = lax.rsqrt(jnp.sum(diag, axis=0, keepdims=True) + EPSILON)
        beta_row = rates_ref[:, part]
        beta_col = jnp.sum(jnp.where(eye, beta_row, 0.0), axis=1, keepdims=True)
        lower = jnp.where(strict, gram * (beta_col * r_col) * r_row, 0.0)
        nmat[b] = lower
        first = jnp.logical_and((ri >> 1) == (ci >> 1), strict)
        inv[b] = jnp.where(eye, 1.0, 0.0) - jnp.where(first, lower, 0.0)
        scales.append((r_col, r_row * beta_row))

    def level(depth, carry):
        near = jnp.logical_and((ri >> (depth + 1)) == (ci >> (depth + 1)), (ri >> depth) != (ci >> depth))
        xs = [inv[b] for b in range(blocks)]
        parts = [split(x) for x in xs]
        ys = []
        for b in range(blocks):
            (mh, ml), (xh, xl) = split(jnp.where(near, nmat[b], 0.0)), parts[b]
            ys.append(mm(mh, xh) + mm(ml, xh) + mm(mh, xl))
        for b in range(blocks):
            (yh, yl), (xh, xl) = split(ys[b]), parts[b]
            inv[b] = xs[b] - (mm(xh, yh) + mm(xl, yh) + mm(xh, yl))
        return carry

    lax.fori_loop(1, block.bit_length() - 1, level, 0)

    fr = lax.broadcasted_iota(jnp.int32, (feat, feat), 0)
    fc = lax.broadcasted_iota(jnp.int32, (feat, feat), 1)
    unit = jnp.where(fr == fc, 1.0, 0.0).astype(F32)
    rights, passages, finals = [], [], []
    for b in range(blocks):
        part = slice(b * block, (b + 1) * block)
        hb, kb = h_ref[part, :], k_ref[part, :]
        r_col, rb_row = scales[b]
        th, tl = split(inv[b] * r_col * rb_row)
        wk = lax.dot_general(hb, kb, nt, preferred_element_type=F32)
        wh, wl = split(jnp.where(strict, wk, 0.0))
        rk = mm(th, wh) + mm(tl, wh) + mm(th, wl)
        rh = mm(th, hb) + mm(tl, hb)
        hbt = hb.astype(F32).T.astype(BF16)
        rkh, rkl = split(rk)
        rhh, rhl = split(rh)
        finals.append(kb.astype(F32).T - (mm(hbt, rkh) + mm(hbt, rkl)))
        passages.append(unit - (mm(hbt, rhh) + mm(hbt, rhl)))
        rights.append((rkh, rkl, rhh, rhl))

    prefixes = [None]
    now = finals[0]
    prefix = passages[0]
    for b in range(1, blocks):
        moved[b - 1, :, : b * block] = now
        prefixes.append(prefix)
        now = jnp.concatenate([dot3(passages[b], now), finals[b]], 1)
        prefix = dot3(passages[b], prefix)
    ksend[...] = now.astype(BF16)
    tsend[...] = prefix
    def both(peer):
        t_copy(me, peer).start()
        k_copy(me, peer).start()
    later(both)

    for b in range(blocks):
        part = slice(b * block, (b + 1) * block)
        hb, kb, qb = h_ref[part, :], k_ref[part, :], q_ref[part, :]
        rkh, rkl, rhh, rhl = rights[b]
        qw = lax.dot_general(qb, hb, nt, preferred_element_type=F32)
        qwh, qwl = split(jnp.where(ri >= ci, qw, 0.0))
        qk = lax.dot_general(qb, kb, nt, preferred_element_type=F32)
        inside = (qk - (mm(qwh, rkh) + mm(qwl, rkh) + mm(qwh, rkl))) * scale
        scores = jnp.where(ri >= ci, inside, NEGATIVE)
        start = (qb.astype(F32) - (mm(qwh, rhh) + mm(qwl, rhh) + mm(qwh, rhl))) * scale
        if b:
            scores = jnp.concatenate([dot3(start, moved[b - 1, :, : b * block]), scores], 1)
            mov[part, :] = dot3(start, prefixes[b])
        else:
            mov[part, :] = start
        top = jnp.max(scores, axis=1, keepdims=True)
        weight = jnp.exp(scores - top)
        peak[part, :] = top
        total[part, :] = jnp.sum(weight, axis=1, keepdims=True)
        acc[part, :] = mm(weight.astype(BF16), v_ref[: (b + 1) * block, :])

    def visit(offset, carry):
        source = me - 1 - offset
        t_copy(source, me).wait_recv()
        k_copy(source, me).wait_recv()
        v_copy(source, me).wait_recv()
        keys = kall[source]
        keys2 = jnp.concatenate([keys, keys], 0)
        vals = vall[source]
        th, tl = split(tall[source])
        th2 = jnp.concatenate([th, th], 0)

        def tile(t, inner):
            part = pl.ds(pl.multiple_of(t * block, block), block)
            qh, ql = split(mov[part, :])
            both = jnp.concatenate([qh, ql], 1)
            scores = mm(both, keys2)
            old = peak[part, :]
            top = jnp.maximum(old, jnp.max(scores, axis=1, keepdims=True))
            weight = jnp.exp(scores - top)
            shrink = jnp.exp(old - top)
            peak[part, :] = top
            total[part, :] = total[part, :] * shrink + jnp.sum(weight, axis=1, keepdims=True)
            acc[part, :] = acc[part, :] * shrink + mm(weight.astype(BF16), vals)
            mov[part, :] = mm(both, th2) + mm(qh, tl)
            return inner

        lax.fori_loop(0, blocks, tile, 0)
        return carry

    lax.fori_loop(0, me, visit, 0)

    att_ref[...] = (acc[...] / total[...]).astype(BF16)
    for step in range(1, n_head):
        a_copy(head, lax.rem(head + step, n_head)).start()
    a_own = pltpu.make_async_copy(
        att_ref, flat_ref.at[:, pl.ds(pl.multiple_of(head * feat, 128), feat)], loc_sem.at[1])
    a_own.start()
    w_own.wait()
    def sent(peer):
        v_copy(me, peer).wait_send()
        t_copy(me, peer).wait_send()
        k_copy(me, peer).wait_send()
    later(sent)
    for step in range(1, n_head):
        other = lax.rem(head + step, n_head)
        w_copy(head, other).wait_send()
        w_copy(other, head).wait_recv()
        a_copy(head, other).wait_send()
        a_copy(other, head).wait_recv()
    a_own.wait()


def solution(mesh):
    n_ctx, n_head = mesh.shape["ctx"], mesh.shape["head"]

    def body(queries, keys, values, house, rates, out_weight):
        rows, _, feat = queries.shape
        block = min(256, rows)
        blocks = rows // block
        width = out_weight.shape[1] // n_head
        vmem = pl.BlockSpec(memory_space=pltpu.VMEM)
        hbm = pl.BlockSpec(memory_space=pl.ANY)
        dma = pltpu.SemaphoreType.DMA
        attended, flat, columns = pl.pallas_call(
            functools.partial(kernel, n_ctx, n_head, block),
            out_shape=(
                jax.ShapeDtypeStruct((rows, feat), BF16),
                jax.ShapeDtypeStruct((rows, n_head * feat), BF16),
                jax.ShapeDtypeStruct((n_head * feat, width), BF16),
            ),
            in_specs=[vmem] * 5 + [hbm],
            out_specs=(vmem, hbm, hbm),
            scratch_shapes=[
                pltpu.VMEM((n_ctx, feat, rows), BF16),
                pltpu.VMEM((n_ctx, rows, feat), BF16),
                pltpu.VMEM((n_ctx, feat, feat), F32),
                pltpu.VMEM((feat, rows), BF16),
                pltpu.VMEM((feat, feat), F32),
                pltpu.VMEM((blocks, block, block), F32),
                pltpu.VMEM((blocks, block, block), F32),
                pltpu.VMEM((max(blocks - 1, 1), feat, rows), F32),
                pltpu.VMEM((rows, feat), F32),
                pltpu.VMEM((rows, feat), F32),
                pltpu.VMEM((rows, 1), F32),
                pltpu.VMEM((rows, 1), F32),
                dma((n_ctx,)), dma((n_ctx,)), dma((n_ctx,)), dma((n_ctx,)), dma((n_ctx,)), dma((n_ctx,)),
                dma((n_head,)), dma((n_head,)), dma((n_head,)), dma((n_head,)), dma((2,)),
            ],
            compiler_params=pltpu.CompilerParams(
                collective_id=0, has_side_effects=True, vmem_limit_bytes=60 * 1024 * 1024),
            name="path_attention",
        )(queries.reshape(rows, feat), keys.reshape(rows, feat), values.reshape(rows, feat),
          house.reshape(rows, feat), rates, out_weight)
        projected = jnp.dot(flat, columns, preferred_element_type=F32)
        return attended.reshape(rows, 1, feat), projected.astype(BF16)

    in_specs = (
        P("ctx", "head", None),
        P("ctx", "head", None),
        P("ctx", "head", None),
        P("ctx", "head", None),
        P("head", "ctx"),
        P("head", None),
    )
    out_specs = (P("ctx", "head", None), P("ctx", "head"))
    return jax.shard_map(body, mesh=mesh, in_specs=in_specs, out_specs=out_specs, check_vma=False)
```
